32 devices in a mesh: gx: 4 (over y, x), gy: 8 (over z, core).
Axes of the slice: x: 2, y: 2, z: 4, core: 2. Of those that a mesh axis runs over, the one named last changes fastest.
Arguments:
- position: float32 [2, 24, 48, 128], P(None, 'gx', 'gy'), may hold values from 0 to 1
- velocity: float32 [2, 24, 48, 128], P(None, 'gx', 'gy'), may hold values from -3 to 3
- other_accel: float32 [2, 24, 48, 128], P(None, 'gx', 'gy'), may hold values from -5 to 5
- phase_ids: int32 [24, 48, 128], P('gx', 'gy'), may hold values from 0 to 1, as said below
- counts: int32 [24, 48], P('gx', 'gy'), may hold values from 48 to 128, as said below
Outputs:
- new_position: float32 [2, 24, 48, 128], P(None, 'gx', 'gy')
- new_velocity: float32 [2, 24, 48, 128], P(None, 'gx', 'gy')
- pressure: float32 [24, 48, 128], P('gx', 'gy')
- monitor: float32 [4, 4], replicated
The draws below stay inside these ranges and needn't reach their ends.
Inputs may be any that keep to these rules, and one draw needn't show every extreme that they name: `counts`: each entry is the number of live slots of its cell; the live slots are the first ones of the cell; some cell holds 128. `phase_ids`: both phases occur among the live slots.
All inputs are finite; a program needn't handle non-finite values.
Results may differ from the reference program's by a relative error of at most 0.0001.
Values sent between devices are 32-bit elements; how exact they have to be, the bound alone decides.
A program may use at most 64 MiB of HBM per device.

```python
import jax
import jax.numpy as jnp
from jax import lax

SLOTS = 128
ITERS = 4
CELLS_X = 24
CELLS_Y = 48


def draw_counts(key, part):
    values = jax.random.randint(key, (CELLS_X, CELLS_Y), 48, SLOTS + 1, dtype=jnp.int32)
    return values.at[0, 0].set(SLOTS)


def draw_phase_ids(key, part):
    values = jax.random.randint(key, (CELLS_X, CELLS_Y, SLOTS), 0, 2, dtype=jnp.int32)
    return values.at[0, 0, 0].set(0).at[0, 0, 1].set(1)


def block_scale(own_key, dims, pieces, smallest, largest):
    factor_of = 1.0
    for axis_at, parts in pieces:
        draws = jax.random.uniform(jax.random.fold_in(jax.random.fold_in(own_key, 6), axis_at), (parts,), jnp.float32, smallest / len(pieces), largest / len(pieces))
        factor_of = factor_of * jnp.repeat(jnp.exp(draws), dims[axis_at] // parts).reshape((-1,) + (1,) * (len(dims) - 1 - axis_at))
    return factor_of


def gaussian(own_key, dims, deviation, reach, split=(), kind=jnp.bfloat16):
    drawn = jax.random.normal(own_key, dims, jnp.float32) * deviation
    if len(split) > 0:
        drawn = block_scale(own_key, dims, split, -0.22, 0.18) * drawn
    return jnp.clip(drawn, min=-reach, max=reach).astype(kind)


def setup_inputs(seed: int = 0) -> dict:
    seeds = jax.random.split(jax.random.key(seed), 6)
    position = jnp.clip(1.0 * jax.random.uniform(seeds[0], (2, CELLS_X, CELLS_Y, SLOTS), jnp.float32) ** block_scale(seeds[0], (2, CELLS_X, CELLS_Y, SLOTS), ((1, 4), (2, 8)), -0.2, 0.2), 0.0, 1.0)
    velocity = gaussian(seeds[1], (2, CELLS_X, CELLS_Y, SLOTS), 0.5, 3.0, ((1, 4), (2, 8)), jnp.float32)
    other_accel = gaussian(seeds[2], (2, CELLS_X, CELLS_Y, SLOTS), 1.0, 5.0, ((1, 4), (2, 8)), jnp.float32)
    phase_ids = draw_phase_ids(jax.random.fold_in(seeds[5], 71), 0)
    counts = draw_counts(jax.random.fold_in(seeds[5], 71), 0)
    return {"position": position, "velocity": velocity, "other_accel": other_accel, "phase_ids": phase_ids, "counts": counts}


TIME_STEP = 0.05
KERNEL_NORM = 4.0 / (3.141592653589793 * 64.0)
REST_LIGHT = 1.2
REST_HEAVY = 1.5
STIFF_LIGHT = 100.0
STIFF_HEAVY = 200.0
MASS_LIGHT = 1.0
MASS_HEAVY = 1.5
SENTINEL = 1.0e30


def window_of(source, off_x, off_y, row_count, col_count):
    return source[1 + off_x:1 + off_x + row_count, 1 + off_y:1 + off_y + col_count]


def pair_sums(centers, padded_list, with_force):
    center_x, center_y = centers[0], centers[1]
    near_x, near_y, near_live = padded_list[0], padded_list[1], padded_list[2]
    row_count, col_count = center_x.shape[0], center_x.shape[1]
    total_a = jnp.zeros_like(center_x)
    total_b = jnp.zeros_like(center_x)
    for off_x in (-1, 0, 1):
        for off_y in (-1, 0, 1):
            other_x = window_of(near_x, off_x, off_y, row_count, col_count)
            other_y = window_of(near_y, off_x, off_y, row_count, col_count)
            other_live = window_of(near_live, off_x, off_y, row_count, col_count)
            diff_x = center_x[..., :, None] - (other_x[..., None, :] + off_x)
            diff_y = center_y[..., :, None] - (other_y[..., None, :] + off_y)
            intersection = jnp.maximum(1.0 - diff_x * diff_x - diff_y * diff_y, 0.0) * other_live[..., None, :]
            if with_force:
                other_term = window_of(padded_list[3], off_x, off_y, row_count, col_count)
                pair_coef = intersection * intersection * (centers[2][..., :, None] + other_term[..., None, :])
                total_a = total_a + jnp.sum(pair_coef * diff_x, axis=-1)
                total_b = total_b + jnp.sum(pair_coef * diff_y, axis=-1)
            else:
                total_a = total_a + jnp.sum(intersection * intersection * intersection, axis=-1)
    if with_force:
        return (total_a, total_b)
    return (total_a,)


def blocked(with_force, centers, padded_list, row_count):
    block_count = row_count // 2

    def one_block(block_index):
        first_row = block_index * 2
        center_part = tuple(lax.dynamic_slice_in_dim(source, first_row, 2, 0) for source in centers)
        padded_part = tuple(lax.dynamic_slice_in_dim(source, first_row, 4, 0) for source in padded_list)
        return pair_sums(center_part, padded_part, with_force)

    results = lax.map(one_block, jnp.arange(block_count, dtype=jnp.int32))
    return tuple(source.reshape((row_count,) + source.shape[2:]) for source in results)


def local_bounds(density_ratio, live_bool, heavy_bool):
    light_sel = live_bool & jnp.logical_not(heavy_bool)
    heavy_sel = live_bool & heavy_bool
    top_ratio = jnp.stack([jnp.max(jnp.where(light_sel, density_ratio, -SENTINEL)),
                           jnp.max(jnp.where(heavy_sel, density_ratio, -SENTINEL))])
    low_ratio = jnp.stack([jnp.min(jnp.where(light_sel, density_ratio, SENTINEL)),
                           jnp.min(jnp.where(heavy_sel, density_ratio, SENTINEL))])
    return top_ratio, low_ratio


def wrapped(source):
    return jnp.pad(source, ((1, 1), (1, 1), (0, 0)), mode="wrap")


def reference(position, velocity, other_accel, phase_ids, counts):
    slot_index = jnp.arange(position.shape[-1], dtype=jnp.int32)
    live_bool = slot_index[None, None, :] < counts[:, :, None]
    heavy_bool = phase_ids == 1
    live_mask = live_bool.astype(jnp.float32)
    rest_density = jnp.where(heavy_bool, REST_HEAVY, REST_LIGHT).astype(jnp.float32)
    stiffness = jnp.where(heavy_bool, STIFF_HEAVY, STIFF_LIGHT).astype(jnp.float32)
    particle_mass = jnp.where(heavy_bool, MASS_HEAVY, MASS_LIGHT).astype(jnp.float32)
    pressure = jnp.zeros_like(live_mask)
    accel_x = jnp.zeros_like(live_mask)
    accel_y = jnp.zeros_like(live_mask)
    monitor_rows = []
    row_total = position.shape[1]
    for iteration in range(ITERS):
        vel_x = velocity[0] + TIME_STEP * (other_accel[0] + accel_x)
        vel_y = velocity[1] + TIME_STEP * (other_accel[1] + accel_y)
        pos_x = position[0] + TIME_STEP * vel_x
        pos_y = position[1] + TIME_STEP * vel_y
        (density_sum,) = blocked(False, (pos_x, pos_y), (wrapped(pos_x), wrapped(pos_y), wrapped(live_mask)), row_total)
        density = KERNEL_NORM * density_sum
        density_ratio = density / rest_density
        top_ratio, low_ratio = local_bounds(density_ratio, live_bool, heavy_bool)
        relaxation = 1.0 / (1.0 + top_ratio - low_ratio)
        particle_relax = jnp.where(heavy_bool, relaxation[1], relaxation[0])
        pressure = live_mask * (pressure + stiffness * particle_relax * (density_ratio - 1.0))
        safe_density = jnp.where(live_bool, density, 1.0)
        press_term = jnp.where(live_bool, pressure / (safe_density * safe_density), 0.0)
        force_x, force_y = blocked(True, (pos_x, pos_y, press_term),
                                   (wrapped(pos_x), wrapped(pos_y), wrapped(live_mask), wrapped(press_term)), row_total)
        accel_x = live_mask * (6.0 * KERNEL_NORM / particle_mass) * force_x
        accel_y = live_mask * (6.0 * KERNEL_NORM / particle_mass) * force_y
        monitor_rows.append(jnp.concatenate([top_ratio, low_ratio]))
    new_vel_x = live_mask * (velocity[0] + TIME_STEP * (other_accel[0] + accel_x))
    new_vel_y = live_mask * (velocity[1] + TIME_STEP * (other_accel[1] + accel_y))
    new_pos_x = live_mask * (position[0] + TIME_STEP * new_vel_x)
    new_pos_y = live_mask * (position[1] + TIME_STEP * new_vel_y)
    return (jnp.stack([new_pos_x, new_pos_y]), jnp.stack([new_vel_x, new_vel_y]), pressure, jnp.stack(monitor_rows))
```

```python
import jax
import jax.numpy as jnp
from jax import lax
from jax.experimental import pallas as pl
from jax.experimental.pallas import tpu as pltpu
from jax.sharding import PartitionSpec as P

ITERS = 4


TIME_STEP = 0.05
KERNEL_NORM = 4.0 / (3.141592653589793 * 64.0)
REST_LIGHT = 1.2
REST_HEAVY = 1.5
STIFF_LIGHT = 100.0
STIFF_HEAVY = 200.0
MASS_LIGHT = 1.0
MASS_HEAVY = 1.5
SENTINEL = 1e30


def padded(block, sides, width):
    for axis, dim in sides:
        count = lax.axis_size(axis)
        forward = [(i, i + 1) for i in range(count - 1)]
        forward.append((count - 1, 0))
        backward = [(target, source) for source, target in forward]
        low = lax.ppermute(
            lax.slice_in_dim(block, block.shape[dim] - width, None, axis=dim), axis, forward
        )
        high = lax.ppermute(lax.slice_in_dim(block, 0, width, axis=dim), axis, backward)
        block = jnp.concatenate([low, block, high], axis=dim)
    return block


EMPTY = -1e30


def split3(value):
    high = value.astype(jnp.bfloat16).astype(jnp.float32)
    rest = value - high
    mid = rest.astype(jnp.bfloat16).astype(jnp.float32)
    low = (rest - mid).astype(jnp.bfloat16).astype(jnp.float32)
    return high, mid, low


def put_rows(ref, row, values, width):
    for at, value in enumerate(values):
        ref[row, at * width : (at + 1) * width, :] = value


def source_features(x, y, live, jf, row, width):
    x = jnp.where(live, x - 0.5, 0.0)
    y = jnp.where(live, y - 0.5, 0.0)
    xh, xm, xl = split3(x)
    yh, ym, yl = split3(y)
    bh, bm, bl = split3(jnp.where(live, -(x * x + y * y), EMPTY))
    one = jnp.ones_like(x)
    nil = jnp.zeros_like(x)
    put_rows(
        jf,
        row,
        [xh, xh, xm, xh, xl, xm, bh, bm, yh, yh, ym, yh, yl, ym, bl, nil]
        + [one, one, one, nil, nil, nil, nil, nil],
        width,
    )


def pair_features(jf, lhs, row, width, half):
    for n in range(width - half):
        first = jf[row, pl.ds(n, 24, stride=width), :]
        second = jf[row, pl.ds(n + half, 24, stride=width), :]
        both = jnp.concatenate([first, second], axis=0)
        lhs[row, n] = both.T.astype(jnp.bfloat16)


def target_features(x, y, xf, yf, af, row, width):
    x = x - 0.5
    y = y - 0.5
    one = jnp.ones_like(x)
    nil = jnp.zeros_like(x)
    for at in range(3):
        h, m, l = split3(2.0 * (x - (at - 1.0)))
        put_rows(xf.at[row], at, [h, m, h, l, h, m, one, one], width)
        h, m, l = split3(2.0 * (y - (at - 1.0)))
        put_rows(yf.at[row], at, [h, m, h, l, h, m, one, nil], width)
    for ax in range(3):
        for ay in range(3):
            dx = x - (ax - 1.0)
            dy = y - (ay - 1.0)
            h, m, l = split3(1.0 - (dx * dx + dy * dy))
            put_rows(af.at[row], 3 * ax + ay, [h, m, l, nil, nil, nil, nil, nil], width)


def target_block(xf, yf, af, row, cell, ax, ay, width):
    return jnp.concatenate(
        [
            xf[row, ax, pl.ds(cell + 1, 8, stride=width), :],
            yf[row, ay, pl.ds(cell + 1, 8, stride=width), :],
            af[row, 3 * ax + ay, pl.ds(cell + 1, 8, stride=width), :],
        ],
        axis=0,
    )


def overlap(lhs, xf, yf, af, row, cell, ax, ay, width, half):
    first = target_block(xf, yf, af, row, cell, ax, ay, width)
    second = target_block(xf, yf, af, row, cell + half, ax, ay, width)
    nil = jnp.zeros_like(first)
    rhs = jnp.concatenate(
        [
            jnp.concatenate([first, nil], axis=1),
            jnp.concatenate([nil, second], axis=1),
        ],
        axis=0,
    ).astype(jnp.bfloat16)
    raw = jnp.dot(lhs[row + ax, cell + ay], rhs, preferred_element_type=jnp.float32)
    return jnp.maximum(raw, 0.0)


def all_features(pos, live, jf, lhs, xf, yf, af, rows, width, half):
    def source_row(row, carry):
        source_features(pos[0, row], pos[1, row], live[row] > 0, jf, row, width)
        pair_features(jf, lhs, row, width, half)
        return carry

    lax.fori_loop(0, rows + 2, source_row, 0)

    def target_row(row, carry):
        target_features(pos[0, row + 1], pos[1, row + 1], xf, yf, af, row, width)
        return carry

    lax.fori_loop(0, rows, target_row, 0)


def density_kernel(pos, live, out, jf, lhs, xf, yf, af):
    rows, cols, slots = out.shape
    width, half = cols + 2, cols // 2
    all_features(pos, live, jf, lhs, xf, yf, af, rows, width, half)

    def one_row(row, carry):
        for cell in range(half):
            total = jnp.zeros((8, 2 * slots), jnp.float32)
            for ax in range(3):
                for ay in range(3):
                    w = overlap(lhs, xf, yf, af, row, cell, ax, ay, width, half)
                    cube = w * w * w
                    total = total + jnp.sum(cube.reshape(slots // 8, 8, 2 * slots), axis=0)
            dens = jnp.sum(total, axis=0, keepdims=True)
            out[row, cell : cell + 1, :] = dens[:, :slots]
            out[row, cell + half : cell + half + 1, :] = dens[:, slots:]
        return carry

    lax.fori_loop(0, rows, one_row, 0)


def value_rows(x, y, term, live, vf, row, width):
    x = jnp.where(live, x - 0.5, 0.0)
    y = jnp.where(live, y - 0.5, 0.0)
    term = jnp.where(live, term, 0.0)
    highs, mids = [], []
    for value in (jnp.ones_like(x), x, y, term, term * x, term * y):
        high, mid, _ = split3(value)
        highs.append(high)
        mids.append(mid)
    nil = jnp.zeros_like(x)
    put_rows(vf, row, highs + [nil, nil] + mids + [nil, nil], width)


def force_kernel(pos, live, term, out, jf, lhs, xf, yf, af, vf, sums):
    _, rows, cols, slots = out.shape
    width, half = cols + 2, cols // 2
    all_features(pos, live, jf, lhs, xf, yf, af, rows, width, half)

    def value_row(row, carry):
        value_rows(pos[0, row], pos[1, row], term[row], live[row] > 0, vf, row, width)
        return carry

    lax.fori_loop(0, rows + 2, value_row, 0)

    def one_row(row, carry):
        for cell in range(half):
            zero = jnp.zeros((8, slots), jnp.float32)
            parts = [[zero, zero, zero], [zero, zero, zero]]
            for ax in range(3):
                for ay in range(3):
                    w = overlap(lhs, xf, yf, af, row, cell, ax, ay, width, half)
                    square = w * w
                    high = square.astype(jnp.bfloat16)
                    low = (square - high.astype(jnp.float32)).astype(jnp.bfloat16)
                    value = jnp.concatenate(
                        [
                            vf[row + ax, pl.ds(cell + ay, 16, stride=width), :],
                            vf[row + ax, pl.ds(cell + ay + half, 16, stride=width), :],
                        ],
                        axis=0,
                    ).astype(jnp.bfloat16)
                    got = jnp.dot(value, high, preferred_element_type=jnp.float32) + jnp.dot(
                        value, low, preferred_element_type=jnp.float32
                    )
                    pieces = (
                        got[0:8, :slots] + got[8:16, :slots],
                        got[16:24, slots:] + got[24:32, slots:],
                    )
                    for acc, piece in zip(parts, pieces):
                        acc[0] = acc[0] + piece
                        if ax != 1:
                            acc[1] = acc[1] + piece if ax == 2 else acc[1] - piece
                        if ay != 1:
                            acc[2] = acc[2] + piece if ay == 2 else acc[2] - piece
            for at, acc in zip((cell, cell + half), parts):
                plain, by_x, by_y = acc
                rows_out = (
                    plain[0:1],
                    plain[1:2] + by_x[0:1],
                    plain[2:3] + by_y[0:1],
                    plain[3:4],
                    plain[4:5] + by_x[3:4],
                    plain[5:6] + by_y[3:4],
                )
                for k, value in enumerate(rows_out):
                    sums[k, at + 1 : at + 2, :] = value
        own_x = pos[0, row + 1] - 0.5
        own_y = pos[1, row + 1] - 0.5
        own_term = term[row + 1]
        force_x = own_term * (own_x * sums[0] - sums[1]) + own_x * sums[3] - sums[4]
        force_y = own_term * (own_y * sums[0] - sums[2]) + own_y * sums[3] - sums[5]
        out[0, row] = force_x[1 : cols + 1]
        out[1, row] = force_y[1 : cols + 1]
        return carry

    lax.fori_loop(0, rows, one_row, 0)


def feature_scratch(rows, cols, slots):
    width, half = cols + 2, cols // 2
    return [
        pltpu.VMEM((rows + 2, 24 * width, slots), jnp.float32),
        pltpu.VMEM((rows + 2, width - half, slots, 48), jnp.bfloat16),
        pltpu.VMEM((rows, 3, 8 * width, slots), jnp.float32),
        pltpu.VMEM((rows, 3, 8 * width, slots), jnp.float32),
        pltpu.VMEM((rows, 9, 8 * width, slots), jnp.float32),
    ]


def density_sums(moved, cycle_mask):
    _, rows, cols, slots = moved.shape
    rows, cols = rows - 2, cols - 2
    return pl.pallas_call(
        density_kernel,
        out_shape=jax.ShapeDtypeStruct((rows, cols, slots), jnp.float32),
        scratch_shapes=feature_scratch(rows, cols, slots),
    )(moved, cycle_mask)


def force_sums(moved, cycle_mask, near_term):
    _, rows, cols, slots = moved.shape
    rows, cols = rows - 2, cols - 2
    return pl.pallas_call(
        force_kernel,
        out_shape=jax.ShapeDtypeStruct((2, rows, cols, slots), jnp.float32),
        scratch_shapes=feature_scratch(rows, cols, slots)
        + [
            pltpu.VMEM((rows + 2, 16 * (cols + 2), slots), jnp.float32),
            pltpu.VMEM((6, cols + 2, slots), jnp.float32),
        ],
    )(moved, cycle_mask, near_term)


def global_bounds(density_ratio, live_bool, heavy_bool):
    light_sel = live_bool & jnp.logical_not(heavy_bool)
    heavy_sel = live_bool & heavy_bool
    top_local = jnp.stack(
        [
            jnp.max(jnp.where(light_sel, density_ratio, -SENTINEL)),
            jnp.max(jnp.where(heavy_sel, density_ratio, -SENTINEL)),
        ]
    )
    low_local = jnp.stack(
        [
            jnp.min(jnp.where(light_sel, density_ratio, SENTINEL)),
            jnp.min(jnp.where(heavy_sel, density_ratio, SENTINEL)),
        ]
    )
    bounds = lax.pmax(jnp.concatenate([top_local, -low_local]), ("gx", "gy"))
    top_ratio = bounds[:2]
    low_ratio = -bounds[2:]
    return (top_ratio, low_ratio)


def phase_params(heavy_bool):
    rest_density = jnp.where(heavy_bool, REST_HEAVY, REST_LIGHT).astype(jnp.float32)
    stiffness = jnp.where(heavy_bool, STIFF_HEAVY, STIFF_LIGHT).astype(jnp.float32)
    return (rest_density, stiffness)


def pressure_update(pressure, density_sum, live_bool, heavy_bool, own_live, own_heavy):
    live_mask = live_bool.astype(jnp.float32)
    rest_density, stiffness = phase_params(heavy_bool)
    density = KERNEL_NORM * density_sum
    density_ratio = density / rest_density
    top_ratio, low_ratio = global_bounds(density_ratio, own_live, own_heavy)
    relaxation = 1.0 / (1.0 + top_ratio - low_ratio)
    particle_relax = jnp.where(heavy_bool, relaxation[1], relaxation[0])
    pressure = live_mask * (pressure + stiffness * particle_relax * (density_ratio - 1.0))
    safe_density = jnp.where(live_bool, density, 1.0)
    press_term = jnp.where(live_bool, pressure / (safe_density * safe_density), 0.0)
    return (pressure, press_term, jnp.concatenate([top_ratio, low_ratio]))


def local(position, velocity, other_accel, phase_ids, counts):
    tile_rows, tile_cols, slot_count = phase_ids.shape
    slot_index = jnp.arange(slot_count, dtype=jnp.int32)
    live_bool = slot_index[None, None, :] < counts[:, :, None]
    heavy_bool = phase_ids == 1
    live_mask = live_bool.astype(jnp.float32)
    particle_mass = jnp.where(heavy_bool, MASS_HEAVY, MASS_LIGHT).astype(jnp.float32)
    slot_codes = jnp.where(live_bool, phase_ids + 1, 0)
    padded_codes = padded(slot_codes, (("gx", 0), ("gy", 1)), 2)
    cycle_codes = padded_codes[1:-1, 1:-1]
    cycle_live = cycle_codes > 0
    cycle_mask = cycle_live.astype(jnp.float32)
    accel_x = jnp.zeros_like(live_mask)
    accel_y = jnp.zeros_like(live_mask)
    monitor_rows = []
    pressure = jnp.zeros_like(live_mask)
    for iteration in range(ITERS):
        vel_x = velocity[0] + TIME_STEP * (other_accel[0] + accel_x)
        vel_y = velocity[1] + TIME_STEP * (other_accel[1] + accel_y)
        pos_x = position[0] + TIME_STEP * vel_x
        pos_y = position[1] + TIME_STEP * vel_y
        moved = padded(jnp.stack([pos_x, pos_y]), (("gx", 1), ("gy", 2)), 1)
        density_sum = density_sums(moved, cycle_mask)
        pressure, press_term, monitor_row = pressure_update(
            pressure, density_sum, live_bool, heavy_bool, live_bool, heavy_bool
        )
        near_term = padded(press_term, (("gx", 0), ("gy", 1)), 1)
        force_x, force_y = force_sums(moved, cycle_mask, near_term)
        accel_x = live_mask * (6.0 * KERNEL_NORM / particle_mass) * force_x
        accel_y = live_mask * (6.0 * KERNEL_NORM / particle_mass) * force_y
        monitor_rows.append(monitor_row)
    new_vel_x = live_mask * (velocity[0] + TIME_STEP * (other_accel[0] + accel_x))
    new_vel_y = live_mask * (velocity[1] + TIME_STEP * (other_accel[1] + accel_y))
    new_pos_x = live_mask * (position[0] + TIME_STEP * new_vel_x)
    new_pos_y = live_mask * (position[1] + TIME_STEP * new_vel_y)
    return (
        jnp.stack([new_pos_x, new_pos_y]),
        jnp.stack([new_vel_x, new_vel_y]),
        pressure,
        jnp.stack(monitor_rows),
    )


def solution(mesh):
    placed = (
        P(None, "gx", "gy", None),
        P(None, "gx", "gy", None),
        P(None, "gx", "gy", None),
        P("gx", "gy", None),
        P("gx", "gy"),
    )
    return jax.shard_map(
        local,
        mesh=mesh,
        in_specs=placed,
        out_specs=(P(None, "gx", "gy", None), P(None, "gx", "gy", None), P("gx", "gy", None), P()),
        check_vma=False,
    )
```

```python
import functools

import jax
import jax.numpy as jnp
from jax import lax
from jax.experimental import pallas as pl
from jax.experimental.pallas import tpu as pltpu
from jax.sharding import PartitionSpec as P

ITERS = 4


TIME_STEP = 0.05
KERNEL_NORM = 4.0 / (3.141592653589793 * 64.0)
REST_LIGHT = 1.2
REST_HEAVY = 1.5
STIFF_LIGHT = 100.0
STIFF_HEAVY = 200.0
MASS_LIGHT = 1.0
MASS_HEAVY = 1.5
SENTINEL = 1e30


EMPTY = -1e30
FAR = 1e30
LIMIT = 1e29
DIRS = tuple((dx, dy) for dx in (-1, 0, 1) for dy in (-1, 0, 1) if dx or dy)


def split3(value):
    high = value.astype(jnp.bfloat16).astype(jnp.float32)
    rest = value - high
    mid = rest.astype(jnp.bfloat16).astype(jnp.float32)
    low = (rest - mid).astype(jnp.bfloat16).astype(jnp.float32)
    return high, mid, low


def put_rows(ref, row, values, width):
    for at, value in enumerate(values):
        ref[row, at * width : (at + 1) * width, :] = value


def source_features(x, y, live, jf, row, width):
    x = jnp.where(live, x - 0.5, 0.0)
    y = jnp.where(live, y - 0.5, 0.0)
    xh, xm, xl = split3(x)
    yh, ym, yl = split3(y)
    bh, bm, bl = split3(jnp.where(live, -(x * x + y * y), EMPTY))
    one = jnp.ones_like(x)
    nil = jnp.zeros_like(x)
    put_rows(
        jf,
        row,
        [xh, xh, xm, xh, xl, xm, bh, bm, yh, yh, ym, yh, yl, ym, bl, nil]
        + [one, one, one, nil, nil, nil, nil, nil],
        width,
    )


def pair_features(jf, lhs, row, width, half):
    for n in range(width - half):
        first = jf[row, pl.ds(n, 24, stride=width), :]
        second = jf[row, pl.ds(n + half, 24, stride=width), :]
        both = jnp.concatenate([first, second], axis=0)
        lhs[row, n] = both.T.astype(jnp.bfloat16)


def target_features(x, y, xf, yf, af, row, width):
    x = jnp.where(x < LIMIT, x, 0.0) - 0.5
    y = y - 0.5
    one = jnp.ones_like(x)
    nil = jnp.zeros_like(x)
    for at in range(3):
        h, m, l = split3(2.0 * (x - (at - 1.0)))
        put_rows(xf.at[row], at, [h, m, h, l, h, m, one, one], width)
        h, m, l = split3(2.0 * (y - (at - 1.0)))
        put_rows(yf.at[row], at, [h, m, h, l, h, m, one, nil], width)
    for ax in range(3):
        for ay in range(3):
            dx = x - (ax - 1.0)
            dy = y - (ay - 1.0)
            h, m, l = split3(1.0 - (dx * dx + dy * dy))
            put_rows(af.at[row], 3 * ax + ay, [h, m, l, nil, nil, nil, nil, nil], width)


def target_block(xf, yf, af, row, cell, ax, ay, width):
    return jnp.concatenate(
        [
            xf[row, ax, pl.ds(cell + 1, 8, stride=width), :],
            yf[row, ay, pl.ds(cell + 1, 8, stride=width), :],
            af[row, 3 * ax + ay, pl.ds(cell + 1, 8, stride=width), :],
        ],
        axis=0,
    )


def overlap(lhs, xf, yf, af, row, cell, ax, ay, width, half):
    first = target_block(xf, yf, af, row, cell, ax, ay, width)
    second = target_block(xf, yf, af, row, cell + half, ax, ay, width)
    nil = jnp.zeros_like(first)
    rhs = jnp.concatenate(
        [
            jnp.concatenate([first, nil], axis=1),
            jnp.concatenate([nil, second], axis=1),
        ],
        axis=0,
    ).astype(jnp.bfloat16)
    raw = jnp.dot(lhs[row + ax, cell + ay], rhs, preferred_element_type=jnp.float32)
    return jnp.maximum(raw, 0.0)


def all_features(pos, jf, lhs, xf, yf, af, rows, width, half):
    def source_row(row, carry):
        source_features(pos[0, row], pos[1, row], pos[0, row] < LIMIT, jf, row, width)
        pair_features(jf, lhs, row, width, half)
        return carry

    lax.fori_loop(0, rows + 2, source_row, 0)

    def target_row(row, carry):
        target_features(pos[0, row + 1], pos[1, row + 1], xf, yf, af, row, width)
        return carry

    lax.fori_loop(0, rows, target_row, 0)


def value_rows(x, y, term, live, vf, row, width):
    x = jnp.where(live, x - 0.5, 0.0)
    y = jnp.where(live, y - 0.5, 0.0)
    term = jnp.where(live, term, 0.0)
    highs, mids = [], []
    for value in (jnp.ones_like(x), x, y, term, term * x, term * y):
        high, mid, _ = split3(value)
        highs.append(high)
        mids.append(mid)
    nil = jnp.zeros_like(x)
    put_rows(vf, row, highs + [nil, nil] + mids + [nil, nil], width)


def density_row(lhs, xf, yf, af, dens, ghi, glo, row, cols, slots):
    width, half = cols + 2, cols // 2
    for cell in range(half):
        total = jnp.zeros((8, 2 * slots), jnp.float32)
        for ax in range(3):
            for ay in range(3):
                w = overlap(lhs, xf, yf, af, row, cell, ax, ay, width, half)
                square = w * w
                high = square.astype(jnp.bfloat16)
                ghi[row, cell, 3 * ax + ay] = high
                glo[row, cell, 3 * ax + ay] = (square - high.astype(jnp.float32)).astype(
                    jnp.bfloat16
                )
                total = total + jnp.sum(
                    (square * w).reshape(slots // 8, 8, 2 * slots), axis=0
                )
        got = jnp.sum(total, axis=0, keepdims=True)
        dens[row, cell + 1 : cell + 2, :] = got[:, :slots]
        dens[row, cell + half + 1 : cell + half + 2, :] = got[:, slots:]


def force_row(vf, ghi, glo, sums, row, cols, slots):
    width, half = cols + 2, cols // 2
    for cell in range(half):
        zero = jnp.zeros((8, slots), jnp.float32)
        parts = [[zero, zero, zero], [zero, zero, zero]]
        for ax in range(3):
            for ay in range(3):
                value = jnp.concatenate(
                    [
                        vf[row + ax, pl.ds(cell + ay, 16, stride=width), :],
                        vf[row + ax, pl.ds(cell + ay + half, 16, stride=width), :],
                    ],
                    axis=0,
                ).astype(jnp.bfloat16)
                got = jnp.dot(
                    value, ghi[row, cell, 3 * ax + ay], preferred_element_type=jnp.float32
                ) + jnp.dot(
                    value, glo[row, cell, 3 * ax + ay], preferred_element_type=jnp.float32
                )
                pieces = (
                    got[0:8, :slots] + got[8:16, :slots],
                    got[16:24, slots:] + got[24:32, slots:],
                )
                for acc, piece in zip(parts, pieces):
                    acc[0] = acc[0] + piece
                    if ax != 1:
                        acc[1] = acc[1] + piece if ax == 2 else acc[1] - piece
                    if ay != 1:
                        acc[2] = acc[2] + piece if ay == 2 else acc[2] - piece
        for at, acc in zip((cell, cell + half), parts):
            plain, by_x, by_y = acc
            rows_out = (
                plain[0:1],
                plain[1:2] + by_x[0:1],
                plain[2:3] + by_y[0:1],
                plain[3:4],
                plain[4:5] + by_x[3:4],
                plain[5:6] + by_y[3:4],
            )
            for k, value in enumerate(rows_out):
                sums[k, at + 1 : at + 2, :] = value


def remote(src, dst, send, recv, to_x, to_y):
    return pltpu.make_async_remote_copy(
        src_ref=src,
        dst_ref=dst,
        send_sem=send,
        recv_sem=recv,
        device_id=(to_x, to_y),
        device_id_type=pl.DeviceIdType.MESH,
    )


def pack_edges(field, out, par, count, rows, cols):
    for d, (dx, dy) in enumerate(DIRS):
        row = rows if dx > 0 else 1
        cell = cols if dy > 0 else 1
        for k in range(count):
            if dy == 0:
                out[par, d, k, : cols + 2, :] = field[k, row]
            elif dx == 0:
                for r in range(1, rows + 1):
                    out[par, d, k, r : r + 1, :] = field[k, r, cell : cell + 1, :]
            else:
                out[par, d, k, 0:1, :] = field[k, row, cell : cell + 1, :]


def unpack_edges(field, got, par, count, rows, cols):
    for d, (dx, dy) in enumerate(DIRS):
        row = 0 if dx > 0 else rows + 1
        cell = 0 if dy > 0 else cols + 1
        for k in range(count):
            if dy == 0:
                field[k, row, 1 : cols + 1, :] = got[par, d, k, 1 : cols + 1, :]
            elif dx == 0:
                for r in range(1, rows + 1):
                    field[k, r, cell : cell + 1, :] = got[par, d, k, r : r + 1, :]
            else:
                field[k, row, cell : cell + 1, :] = got[par, d, k, 0:1, :]


def step_kernel(
    nx, ny,
    pos_in, vel_in, oth_in, code_in,
    pos_out, vel_out, press_out, bounds_out,
    base, pos, acc, press, parts, ratio, dens,
    jf, lhs, xf, yf, af, vf, sums, ghi, glo,
    pos_snd, pos_rcv, ab_snd, ab_rcv, one_snd, one_rcv, two_snd, two_rcv,
    pos_ss, pos_rs, ab_ss, ab_rs, one_ss, one_rs, two_ss, two_rs,
):
    _, rows, cols, slots = pos_in.shape
    width, half = cols + 2, cols // 2
    me_x, me_y = lax.axis_index("gx"), lax.axis_index("gy")

    def at_x(step):
        return lax.rem(me_x + step + nx, nx)

    def at_y(step):
        return lax.rem(me_y + step + ny, ny)

    barrier = pltpu.get_barrier_semaphore()
    partners = [(0, k) for k in range(1, ny)] + [(k, 0) for k in range(1, nx)]
    partners += [(dx, dy) for dx, dy in DIRS if dx and dy]
    for dx, dy in partners:
        pl.semaphore_signal(
            barrier, inc=1, device_id=(at_x(dx), at_y(dy)), device_id_type=pl.DeviceIdType.MESH
        )

    for ref in (base, acc, press, ratio, dens, sums, parts, pos):
        ref[...] = jnp.zeros_like(ref)
    for ref in (pos_snd, ab_snd):
        ref[...] = jnp.zeros_like(ref)
    for row in range(rows):
        for k, source in enumerate((pos_in, vel_in, oth_in)):
            for c in range(2):
                base[2 * k + c, row, 1 : cols + 1, :] = source[c, row]
        base[6, row, 1 : cols + 1, :] = code_in[row]
    pl.semaphore_wait(barrier, len(partners))

    def halo(src, dst, send, recv, par):
        return [
            remote(src.at[par, d], dst.at[par, d], send.at[par, d], recv.at[par, d], at_x(dx), at_y(dy))
            for d, (dx, dy) in enumerate(DIRS)
        ]

    def one_iteration(it, carry):
        par = lax.rem(it, 2)

        def predict(row, carry):
            live = base[6, row] > 0
            for c in range(2):
                vel = base[2 + c, row] + TIME_STEP * (base[4 + c, row] + acc[c, row])
                moved = base[c, row] + TIME_STEP * vel
                pos[c, row + 1] = jnp.where(live, moved, FAR if c == 0 else 0.0)
            return carry

        lax.fori_loop(0, rows, predict, 0)
        pack_edges(pos, pos_snd, par, 2, rows, cols)
        copies = halo(pos_snd, pos_rcv, pos_ss, pos_rs, par)
        for copy in copies:
            copy.start()
        for copy in copies:
            copy.wait()
        unpack_edges(pos, pos_rcv, par, 2, rows, cols)

        all_features(pos, jf, lhs, xf, yf, af, rows, width, half)

        def density_step(row, carry):
            density_row(lhs, xf, yf, af, dens, ghi, glo, row, cols, slots)
            return carry

        lax.fori_loop(0, rows, density_step, 0)

        def bounds_step(row, carry):
            code = base[6, row]
            live = code > 0.5
            heavy = code > 1.5
            density = KERNEL_NORM * dens[row]
            own = density / jnp.where(heavy, REST_HEAVY, REST_LIGHT)
            ratio[row] = own
            safe = jnp.where(live, density, 1.0)
            alpha = jnp.where(live, press[row] / (safe * safe), 0.0)
            stiff = jnp.where(heavy, STIFF_HEAVY, STIFF_LIGHT)
            beta = jnp.where(live, stiff * (own - 1.0) / (safe * safe), 0.0)
            parts[0, row + 1] = alpha
            parts[1, row + 1] = jnp.where(heavy, 0.0, beta)
            parts[2, row + 1] = jnp.where(heavy, beta, 0.0)
            light_sel = live & jnp.logical_not(heavy)
            heavy_sel = live & heavy
            return (
                jnp.maximum(carry[0], jnp.where(light_sel, own, -SENTINEL)),
                jnp.maximum(carry[1], jnp.where(heavy_sel, own, -SENTINEL)),
                jnp.maximum(carry[2], jnp.where(light_sel, -own, -SENTINEL)),
                jnp.maximum(carry[3], jnp.where(heavy_sel, -own, -SENTINEL)),
            )

        floor = jnp.full((width, slots), -SENTINEL, jnp.float32)
        local = lax.fori_loop(0, rows, bounds_step, (floor,) * 4)
        for k, value in enumerate(local):
            one_snd[par, k : k + 1, :] = jnp.max(value, axis=0, keepdims=True)
        one_snd[par, 4:8, :] = jnp.full((4, slots), -SENTINEL, jnp.float32)
        firsts = [
            remote(one_snd.at[par], one_rcv.at[par, k], one_ss.at[par, k], one_rs.at[par, k], me_x, at_y(k))
            for k in range(1, ny)
        ]
        for copy in firsts:
            copy.start()
        pack_edges(parts, ab_snd, par, 3, rows, cols)
        copies = halo(ab_snd, ab_rcv, ab_ss, ab_rs, par)
        for copy in copies:
            copy.start()
        for copy in firsts:
            copy.wait()
        best = one_snd[par]
        for k in range(1, ny):
            best = jnp.maximum(best, one_rcv[par, k])
        two_snd[par] = best
        seconds = [
            remote(two_snd.at[par], two_rcv.at[par, k], two_ss.at[par, k], two_rs.at[par, k], at_x(k), me_y)
            for k in range(1, nx)
        ]
        for copy in seconds:
            copy.start()
        for copy in copies:
            copy.wait()
        unpack_edges(parts, ab_rcv, par, 3, rows, cols)
        for copy in seconds:
            copy.wait()
        for k in range(1, nx):
            best = jnp.maximum(best, two_rcv[par, k])
        bound = jnp.max(best, axis=1, keepdims=True)
        bounds_out[it] = jnp.broadcast_to(bound, (8, slots))
        relax = 1.0 / (1.0 + bound[0:2] + bound[2:4])
        relax_light = relax[0:1]
        relax_heavy = relax[1:2]

        def term_step(row, carry):
            term = parts[0, row] + relax_light * parts[1, row] + relax_heavy * parts[2, row]
            value_rows(pos[0, row], pos[1, row], term, pos[0, row] < LIMIT, vf, row, width)
            return carry

        lax.fori_loop(0, rows + 2, term_step, 0)

        def force_step(row, carry):
            force_row(vf, ghi, glo, sums, row, cols, slots)
            code = base[6, row]
            live = code > 0.5
            heavy = code > 1.5
            relaxed = jnp.where(heavy, STIFF_HEAVY * relax_heavy, STIFF_LIGHT * relax_light)
            press[row] = jnp.where(live, press[row] + relaxed * (ratio[row] - 1.0), 0.0)
            term = (
                parts[0, row + 1]
                + relax_light * parts[1, row + 1]
                + relax_heavy * parts[2, row + 1]
            )
            scale = jnp.where(
                heavy, 6.0 * KERNEL_NORM / MASS_HEAVY, 6.0 * KERNEL_NORM / MASS_LIGHT
            )
            for c in range(2):
                own = pos[c, row + 1] - 0.5
                force = term * (own * sums[0] - sums[1 + c]) + own * sums[3] - sums[4 + c]
                acc[c, row] = jnp.where(live, scale * force, 0.0)
            return carry

        lax.fori_loop(0, rows, force_step, 0)
        return carry

    lax.fori_loop(0, ITERS, one_iteration, 0)

    def finish(row, carry):
        live = base[6, row] > 0.5
        press_out[row] = press[row, 1 : cols + 1, :]
        for c in range(2):
            vel = base[2 + c, row] + TIME_STEP * (base[4 + c, row] + acc[c, row])
            vel = jnp.where(live, vel, 0.0)
            place = jnp.where(live, base[c, row] + TIME_STEP * vel, 0.0)
            vel_out[c, row] = vel[1 : cols + 1]
            pos_out[c, row] = place[1 : cols + 1]
        return carry

    lax.fori_loop(0, rows, finish, 0)


def local(position, velocity, other_accel, phase_ids, counts):
    rows, cols, slots = phase_ids.shape
    width, half = cols + 2, cols // 2
    nx, ny = lax.axis_size("gx"), lax.axis_size("gy")
    high = max(width, rows + 2)
    slot_index = jnp.arange(slots, dtype=jnp.int32)
    live = slot_index[None, None, :] < counts[:, :, None]
    codes = jnp.where(live, phase_ids + 1, 0).astype(jnp.float32)

    def vm(*shape):
        return pltpu.VMEM(shape, jnp.float32)

    def half_vm(*shape):
        return pltpu.VMEM(shape, jnp.bfloat16)

    dma = pltpu.SemaphoreType.DMA
    new_pos, new_vel, pressure, bounds = pl.pallas_call(
        functools.partial(step_kernel, nx, ny),
        out_shape=(
            jax.ShapeDtypeStruct((2, rows, cols, slots), jnp.float32),
            jax.ShapeDtypeStruct((2, rows, cols, slots), jnp.float32),
            jax.ShapeDtypeStruct((rows, cols, slots), jnp.float32),
            jax.ShapeDtypeStruct((ITERS, 8, slots), jnp.float32),
        ),
        in_specs=[pl.BlockSpec(memory_space=pltpu.VMEM)] * 4,
        out_specs=(pl.BlockSpec(memory_space=pltpu.VMEM),) * 4,
        scratch_shapes=[
            vm(7, rows, width, slots),
            vm(2, rows + 2, width, slots),
            vm(2, rows, width, slots),
            vm(rows, width, slots),
            vm(3, rows + 2, width, slots),
            vm(rows, width, slots),
            vm(rows, width, slots),
            vm(rows + 2, 24 * width, slots),
            half_vm(rows + 2, width - half, slots, 48),
            vm(rows, 3, 8 * width, slots),
            vm(rows, 3, 8 * width, slots),
            vm(rows, 9, 8 * width, slots),
            vm(rows + 2, 16 * width, slots),
            vm(6, width, slots),
            half_vm(rows, half, 9, slots, 2 * slots),
            half_vm(rows, half, 9, slots, 2 * slots),
            vm(2, 8, 2, high, slots),
            vm(2, 8, 2, high, slots),
            vm(2, 8, 3, high, slots),
            vm(2, 8, 3, high, slots),
            vm(2, 8, slots),
            vm(2, ny, 8, slots),
            vm(2, 8, slots),
            vm(2, nx, 8, slots),
            dma((2, 8)), dma((2, 8)), dma((2, 8)), dma((2, 8)),
            dma((2, ny)), dma((2, ny)), dma((2, nx)), dma((2, nx)),
        ],
        compiler_params=pltpu.CompilerParams(collective_id=0, has_side_effects=True),
    )(position, velocity, other_accel, codes)
    tops = bounds[:, :2, 0]
    lows = -bounds[:, 2:4, 0]
    return new_pos, new_vel, pressure, jnp.concatenate([tops, lows], axis=1)


def solution(mesh):
    placed = (
        P(None, "gx", "gy", None),
        P(None, "gx", "gy", None),
        P(None, "gx", "gy", None),
        P("gx", "gy", None),
        P("gx", "gy"),
    )
    return jax.shard_map(
        local,
        mesh=mesh,
        in_specs=placed,
        out_specs=(P(None, "gx", "gy", None), P(None, "gx", "gy", None), P("gx", "gy", None), P()),
        check_vma=False,
    )
```

```python
import functools

import jax
import jax.numpy as jnp
from jax import lax
from jax.experimental import pallas as pl
from jax.experimental.pallas import tpu as pltpu
from jax.sharding import PartitionSpec as P

ITERS = 4


TIME_STEP = 0.05
KERNEL_NORM = 4.0 / (3.141592653589793 * 64.0)
REST_LIGHT = 1.2
REST_HEAVY = 1.5
STIFF_LIGHT = 100.0
STIFF_HEAVY = 200.0
MASS_LIGHT = 1.0
MASS_HEAVY = 1.5
SENTINEL = 1e30


EMPTY = -1e30
FAR = 1e30
LIMIT = 1e29
DIRS = tuple((dx, dy) for dx in (-1, 0, 1) for dy in (-1, 0, 1) if dx or dy)


def split3(value):
    high = value.astype(jnp.bfloat16).astype(jnp.float32)
    rest = value - high
    mid = rest.astype(jnp.bfloat16).astype(jnp.float32)
    low = (rest - mid).astype(jnp.bfloat16).astype(jnp.float32)
    return high, mid, low


def put_rows(ref, row, values, width):
    for at, value in enumerate(values):
        ref[row, at * width : (at + 1) * width, :] = value


def source_features(x, y, live, jf, row, width):
    x = jnp.where(live, x - 0.5, 0.0)
    y = jnp.where(live, y - 0.5, 0.0)
    xh, xm, xl = split3(x)
    yh, ym, yl = split3(y)
    bh, bm, bl = split3(jnp.where(live, -(x * x + y * y), EMPTY))
    one = jnp.ones_like(x)
    nil = jnp.zeros_like(x)
    put_rows(
        jf,
        row,
        [xh, xh, xm, xh, xl, xm, bh, bm, yh, yh, ym, yh, yl, ym, bl, nil]
        + [one, one, one, nil, nil, nil, nil, nil],
        width,
    )


def pair_features(jf, lhs, row, width, half):
    for n in range(width - half):
        first = jf[row, pl.ds(n, 24, stride=width), :]
        second = jf[row, pl.ds(n + half, 24, stride=width), :]
        both = jnp.concatenate([first, second], axis=0)
        lhs[row, n] = both.T.astype(jnp.bfloat16)


def target_features(x, y, xf, yf, af, row, width):
    x = jnp.where(x < LIMIT, x, 0.0) - 0.5
    y = y - 0.5
    one = jnp.ones_like(x)
    nil = jnp.zeros_like(x)
    for at in range(3):
        h, m, l = split3(2.0 * (x - (at - 1.0)))
        put_rows(xf.at[row], at, [h, m, h, l, h, m, one, one], width)
        h, m, l = split3(2.0 * (y - (at - 1.0)))
        put_rows(yf.at[row], at, [h, m, h, l, h, m, one, nil], width)
    for ax in range(3):
        for ay in range(3):
            dx = x - (ax - 1.0)
            dy = y - (ay - 1.0)
            h, m, l = split3(1.0 - (dx * dx + dy * dy))
            put_rows(af.at[row], 3 * ax + ay, [h, m, l, nil, nil, nil, nil, nil], width)


def target_block(xf, yf, af, row, cell, ax, ay, width):
    return jnp.concatenate(
        [
            xf[row, ax, pl.ds(cell + 1, 8, stride=width), :],
            yf[row, ay, pl.ds(cell + 1, 8, stride=width), :],
            af[row, 3 * ax + ay, pl.ds(cell + 1, 8, stride=width), :],
        ],
        axis=0,
    )


def overlap(lhs, xf, yf, af, row, cell, ax, ay, width, half):
    first = target_block(xf, yf, af, row, cell, ax, ay, width)
    second = target_block(xf, yf, af, row, cell + half, ax, ay, width)
    nil = jnp.zeros_like(first)
    rhs = jnp.concatenate(
        [
            jnp.concatenate([first, nil], axis=1),
            jnp.concatenate([nil, second], axis=1),
        ],
        axis=0,
    ).astype(jnp.bfloat16)
    raw = jnp.dot(lhs[row + ax, cell + ay], rhs, preferred_element_type=jnp.float32)
    return jnp.maximum(raw, 0.0)


def all_sources(pos, jf, lhs, rows, width, half):
    def source_row(row, carry):
        source_features(pos[0, row], pos[1, row], pos[0, row] < LIMIT, jf, row, width)
        pair_features(jf, lhs, row, width, half)
        return carry

    lax.fori_loop(0, rows + 2, source_row, 0)


def all_targets(pos, xf, yf, af, rows, width):
    def target_row(row, carry):
        target_features(pos[0, row + 1], pos[1, row + 1], xf, yf, af, row, width)
        return carry

    lax.fori_loop(0, rows, target_row, 0)


def value_rows(x, y, term, live, vf, row, width):
    x = jnp.where(live, x - 0.5, 0.0)
    y = jnp.where(live, y - 0.5, 0.0)
    term = jnp.where(live, term, 0.0)
    highs, mids = [], []
    for value in (jnp.ones_like(x), x, y, term, term * x, term * y):
        high, mid, _ = split3(value)
        highs.append(high)
        mids.append(mid)
    nil = jnp.zeros_like(x)
    put_rows(vf, row, highs + [nil, nil] + mids + [nil, nil], width)


def density_row(lhs, xf, yf, af, dens, gain, row, cols, slots):
    width, half = cols + 2, cols // 2
    for cell in range(half):
        total = jnp.zeros((8, 2 * slots), jnp.float32)
        for ax in range(3):
            for ay in range(3):
                w = overlap(lhs, xf, yf, af, row, cell, ax, ay, width, half)
                square = w * w
                high = square.astype(jnp.bfloat16)
                gain[row, cell, 3 * ax + ay, :slots, :] = high
                gain[row, cell, 3 * ax + ay, slots:, :] = (
                    square - high.astype(jnp.float32)
                ).astype(jnp.bfloat16)
                total = total + jnp.sum(
                    (square * w).reshape(slots // 8, 8, 2 * slots), axis=0
                )
        got = jnp.sum(total, axis=0, keepdims=True)
        dens[row, cell + 1 : cell + 2, :] = got[:, :slots]
        dens[row, cell + half + 1 : cell + half + 2, :] = got[:, slots:]


def force_row(vf, gain, sums, row, cols, slots):
    width, half = cols + 2, cols // 2
    for cell in range(half):
        zero = jnp.zeros((8, slots), jnp.float32)
        parts = [[zero, zero, zero], [zero, zero, zero]]
        for ax in range(3):
            for ay in range(3):
                value = jnp.concatenate(
                    [
                        vf[row + ax, pl.ds(cell + ay, 16, stride=width), :],
                        vf[row + ax, pl.ds(cell + ay + half, 16, stride=width), :],
                    ],
                    axis=0,
                ).astype(jnp.bfloat16)
                got = jnp.dot(
                    jnp.concatenate([value, value], axis=1),
                    gain[row, cell, 3 * ax + ay],
                    preferred_element_type=jnp.float32,
                )
                pieces = (
                    got[0:8, :slots] + got[8:16, :slots],
                    got[16:24, slots:] + got[24:32, slots:],
                )
                for acc, piece in zip(parts, pieces):
                    acc[0] = acc[0] + piece
                    if ax != 1:
                        acc[1] = acc[1] + piece if ax == 2 else acc[1] - piece
                    if ay != 1:
                        acc[2] = acc[2] + piece if ay == 2 else acc[2] - piece
        for at, acc in zip((cell, cell + half), parts):
            plain, by_x, by_y = acc
            rows_out = (
                plain[0:1],
                plain[1:2] + by_x[0:1],
                plain[2:3] + by_y[0:1],
                plain[3:4],
                plain[4:5] + by_x[3:4],
                plain[5:6] + by_y[3:4],
            )
            for k, value in enumerate(rows_out):
                sums[k, at + 1 : at + 2, :] = value


def remote(src, dst, send, recv, to_x, to_y):
    return pltpu.make_async_remote_copy(
        src_ref=src,
        dst_ref=dst,
        send_sem=send,
        recv_sem=recv,
        device_id=(to_x, to_y),
        device_id_type=pl.DeviceIdType.MESH,
    )


def pack_edges(field, out, par, count, rows, cols):
    for d, (dx, dy) in enumerate(DIRS):
        row = rows if dx > 0 else 1
        cell = cols if dy > 0 else 1
        for k in range(count):
            if dy == 0:
                out[par, d, k, : cols + 2, :] = field[k, row]
            elif dx == 0:
                for r in range(1, rows + 1):
                    out[par, d, k, r : r + 1, :] = field[k, r, cell : cell + 1, :]
            else:
                out[par, d, k, 0:1, :] = field[k, row, cell : cell + 1, :]


def unpack_edges(field, got, par, count, rows, cols):
    for d, (dx, dy) in enumerate(DIRS):
        row = 0 if dx > 0 else rows + 1
        cell = 0 if dy > 0 else cols + 1
        for k in range(count):
            if dy == 0:
                field[k, row, 1 : cols + 1, :] = got[par, d, k, 1 : cols + 1, :]
            elif dx == 0:
                for r in range(1, rows + 1):
                    field[k, r, cell : cell + 1, :] = got[par, d, k, r : r + 1, :]
            else:
                field[k, row, cell : cell + 1, :] = got[par, d, k, 0:1, :]


def step_kernel(
    nx, ny,
    pos_in, vel_in, oth_in, code_in,
    pos_out, vel_out, press_out, bounds_out,
    base, pos, acc, press, parts, ratio, dens,
    jf, lhs, xf, yf, af, vf, sums, gain,
    pos_snd, pos_rcv, ab_snd, ab_rcv, one_snd, one_rcv, two_snd, two_rcv,
    pos_ss, pos_rs, ab_ss, ab_rs, one_ss, one_rs, two_ss, two_rs,
):
    _, rows, cols, slots = pos_in.shape
    width, half = cols + 2, cols // 2
    me_x, me_y = lax.axis_index("gx"), lax.axis_index("gy")

    def at_x(step):
        return lax.rem(me_x + step + nx, nx)

    def at_y(step):
        return lax.rem(me_y + step + ny, ny)

    barrier = pltpu.get_barrier_semaphore()
    partners = [(0, k) for k in range(1, ny)] + [(k, 0) for k in range(1, nx)]
    partners += [(dx, dy) for dx, dy in DIRS if dx and dy]
    for dx, dy in partners:
        pl.semaphore_signal(
            barrier, inc=1, device_id=(at_x(dx), at_y(dy)), device_id_type=pl.DeviceIdType.MESH
        )

    for ref in (base, acc, press, ratio, dens, sums, parts, pos):
        ref[...] = jnp.zeros_like(ref)
    for ref in (pos_snd, ab_snd):
        ref[...] = jnp.zeros_like(ref)
    for row in range(rows):
        for k, source in enumerate((pos_in, vel_in, oth_in)):
            for c in range(2):
                base[2 * k + c, row, 1 : cols + 1, :] = source[c, row]
        base[6, row, 1 : cols + 1, :] = code_in[row]
    pl.semaphore_wait(barrier, len(partners))

    def halo(src, dst, send, recv, par):
        return [
            remote(src.at[par, d], dst.at[par, d], send.at[par, d], recv.at[par, d], at_x(dx), at_y(dy))
            for d, (dx, dy) in enumerate(DIRS)
        ]

    def one_iteration(it, carry):
        par = lax.rem(it, 2)

        def predict(row, carry):
            live = base[6, row] > 0
            for c in range(2):
                vel = base[2 + c, row] + TIME_STEP * (base[4 + c, row] + acc[c, row])
                moved = base[c, row] + TIME_STEP * vel
                pos[c, row + 1] = jnp.where(live, moved, FAR if c == 0 else 0.0)
            return carry

        lax.fori_loop(0, rows, predict, 0)
        pack_edges(pos, pos_snd, par, 2, rows, cols)
        copies = halo(pos_snd, pos_rcv, pos_ss, pos_rs, par)
        for copy in copies:
            copy.start()
        all_targets(pos, xf, yf, af, rows, width)
        for copy in copies:
            copy.wait()
        unpack_edges(pos, pos_rcv, par, 2, rows, cols)

        all_sources(pos, jf, lhs, rows, width, half)

        def density_step(row, carry):
            density_row(lhs, xf, yf, af, dens, gain, row, cols, slots)
            return carry

        lax.fori_loop(0, rows, density_step, 0)

        def bounds_step(row, carry):
            code = base[6, row]
            live = code > 0.5
            heavy = code > 1.5
            density = KERNEL_NORM * dens[row]
            own = density / jnp.where(heavy, REST_HEAVY, REST_LIGHT)
            ratio[row] = own
            safe = jnp.where(live, density, 1.0)
            alpha = jnp.where(live, press[row] / (safe * safe), 0.0)
            stiff = jnp.where(heavy, STIFF_HEAVY, STIFF_LIGHT)
            beta = jnp.where(live, stiff * (own - 1.0) / (safe * safe), 0.0)
            parts[0, row + 1] = alpha
            parts[1, row + 1] = jnp.where(heavy, 0.0, beta)
            parts[2, row + 1] = jnp.where(heavy, beta, 0.0)
            light_sel = live & jnp.logical_not(heavy)
            heavy_sel = live & heavy
            return (
                jnp.maximum(carry[0], jnp.where(light_sel, own, -SENTINEL)),
                jnp.maximum(carry[1], jnp.where(heavy_sel, own, -SENTINEL)),
                jnp.maximum(carry[2], jnp.where(light_sel, -own, -SENTINEL)),
                jnp.maximum(carry[3], jnp.where(heavy_sel, -own, -SENTINEL)),
            )

        floor = jnp.full((width, slots), -SENTINEL, jnp.float32)
        local = lax.fori_loop(0, rows, bounds_step, (floor,) * 4)
        for k, value in enumerate(local):
            one_snd[par, k : k + 1, :] = jnp.max(value, axis=0, keepdims=True)
        one_snd[par, 4:8, :] = jnp.full((4, slots), -SENTINEL, jnp.float32)
        firsts = [
            remote(one_snd.at[par], one_rcv.at[par, k], one_ss.at[par, k], one_rs.at[par, k], me_x, at_y(k))
            for k in range(1, ny)
        ]
        for copy in firsts:
            copy.start()
        pack_edges(parts, ab_snd, par, 3, rows, cols)
        copies = halo(ab_snd, ab_rcv, ab_ss, ab_rs, par)
        for copy in copies:
            copy.start()
        for copy in firsts:
            copy.wait()
        best = one_snd[par]
        for k in range(1, ny):
            best = jnp.maximum(best, one_rcv[par, k])
        two_snd[par] = best
        seconds = [
            remote(two_snd.at[par], two_rcv.at[par, k], two_ss.at[par, k], two_rs.at[par, k], at_x(k), me_y)
            for k in range(1, nx)
        ]
        for copy in seconds:
            copy.start()
        for copy in copies:
            copy.wait()
        unpack_edges(parts, ab_rcv, par, 3, rows, cols)
        for copy in seconds:
            copy.wait()
        for k in range(1, nx):
            best = jnp.maximum(best, two_rcv[par, k])
        bound = jnp.max(best, axis=1, keepdims=True)
        bounds_out[it] = jnp.broadcast_to(bound, (8, slots))
        relax = 1.0 / (1.0 + bound[0:2] + bound[2:4])
        relax_light = relax[0:1]
        relax_heavy = relax[1:2]

        def term_step(row, carry):
            term = parts[0, row] + relax_light * parts[1, row] + relax_heavy * parts[2, row]
            value_rows(pos[0, row], pos[1, row], term, pos[0, row] < LIMIT, vf, row, width)
            return carry

        lax.fori_loop(0, rows + 2, term_step, 0)

        def force_step(row, carry):
            force_row(vf, gain, sums, row, cols, slots)
            code = base[6, row]
            live = code > 0.5
            heavy = code > 1.5
            relaxed = jnp.where(heavy, STIFF_HEAVY * relax_heavy, STIFF_LIGHT * relax_light)
            press[row] = jnp.where(live, press[row] + relaxed * (ratio[row] - 1.0), 0.0)
            term = (
                parts[0, row + 1]
                + relax_light * parts[1, row + 1]
                + relax_heavy * parts[2, row + 1]
            )
            scale = jnp.where(
                heavy, 6.0 * KERNEL_NORM / MASS_HEAVY, 6.0 * KERNEL_NORM / MASS_LIGHT
            )
            for c in range(2):
                own = pos[c, row + 1] - 0.5
                force = term * (own * sums[0] - sums[1 + c]) + own * sums[3] - sums[4 + c]
                acc[c, row] = jnp.where(live, scale * force, 0.0)
            return carry

        lax.fori_loop(0, rows, force_step, 0)
        return carry

    lax.fori_loop(0, ITERS, one_iteration, 0)

    def finish(row, carry):
        live = base[6, row] > 0.5
        press_out[row] = press[row, 1 : cols + 1, :]
        for c in range(2):
            vel = base[2 + c, row] + TIME_STEP * (base[4 + c, row] + acc[c, row])
            vel = jnp.where(live, vel, 0.0)
            place = jnp.where(live, base[c, row] + TIME_STEP * vel, 0.0)
            vel_out[c, row] = vel[1 : cols + 1]
            pos_out[c, row] = place[1 : cols + 1]
        return carry

    lax.fori_loop(0, rows, finish, 0)


def local(position, velocity, other_accel, phase_ids, counts):
    rows, cols, slots = phase_ids.shape
    width, half = cols + 2, cols // 2
    nx, ny = lax.axis_size("gx"), lax.axis_size("gy")
    high = max(width, rows + 2)
    slot_index = jnp.arange(slots, dtype=jnp.int32)
    live = slot_index[None, None, :] < counts[:, :, None]
    codes = jnp.where(live, phase_ids + 1, 0).astype(jnp.float32)

    def vm(*shape):
        return pltpu.VMEM(shape, jnp.float32)

    def half_vm(*shape):
        return pltpu.VMEM(shape, jnp.bfloat16)

    dma = pltpu.SemaphoreType.DMA
    new_pos, new_vel, pressure, bounds = pl.pallas_call(
        functools.partial(step_kernel, nx, ny),
        out_shape=(
            jax.ShapeDtypeStruct((2, rows, cols, slots), jnp.float32),
            jax.ShapeDtypeStruct((2, rows, cols, slots), jnp.float32),
            jax.ShapeDtypeStruct((rows, cols, slots), jnp.float32),
            jax.ShapeDtypeStruct((ITERS, 8, slots), jnp.float32),
        ),
        in_specs=[pl.BlockSpec(memory_space=pltpu.VMEM)] * 4,
        out_specs=(pl.BlockSpec(memory_space=pltpu.VMEM),) * 4,
        scratch_shapes=[
            vm(7, rows, width, slots),
            vm(2, rows + 2, width, slots),
            vm(2, rows, width, slots),
            vm(rows, width, slots),
            vm(3, rows + 2, width, slots),
            vm(rows, width, slots),
            vm(rows, width, slots),
            vm(rows + 2, 24 * width, slots),
            half_vm(rows + 2, width - half, slots, 48),
            vm(rows, 3, 8 * width, slots),
            vm(rows, 3, 8 * width, slots),
            vm(rows, 9, 8 * width, slots),
            vm(rows + 2, 16 * width, slots),
            vm(6, width, slots),
            half_vm(rows, half, 9, 2 * slots, 2 * slots),
            vm(2, 8, 2, high, slots),
            vm(2, 8, 2, high, slots),
            vm(2, 8, 3, high, slots),
            vm(2, 8, 3, high, slots),
            vm(2, 8, slots),
            vm(2, ny, 8, slots),
            vm(2, 8, slots),
            vm(2, nx, 8, slots),
            dma((2, 8)), dma((2, 8)), dma((2, 8)), dma((2, 8)),
            dma((2, ny)), dma((2, ny)), dma((2, nx)), dma((2, nx)),
        ],
        compiler_params=pltpu.CompilerParams(collective_id=0, has_side_effects=True),
    )(position, velocity, other_accel, codes)
    tops = bounds[:, :2, 0]
    lows = -bounds[:, 2:4, 0]
    return new_pos, new_vel, pressure, jnp.concatenate([tops, lows], axis=1)


def solution(mesh):
    placed = (
        P(None, "gx", "gy", None),
        P(None, "gx", "gy", None),
        P(None, "gx", "gy", None),
        P("gx", "gy", None),
        P("gx", "gy"),
    )
    return jax.shard_map(
        local,
        mesh=mesh,
        in_specs=placed,
        out_specs=(P(None, "gx", "gy", None), P(None, "gx", "gy", None), P("gx", "gy", None), P()),
        check_vma=False,
    )
```
